128 devices in a mesh: grid: 16 (over y, z_lo, core), dom: 8 (over x, z_hi).
Axes of the slice: x: 4, y: 4, z: 4 (z_hi: 2, z_lo: 2; z = z_hi * 2 + z_lo), core: 2. Of those that a mesh axis runs over, the one named last changes fastest.
Arguments:
- values: float32 [16, 32, 4, 4, 8, 8, 128], P('grid', 'dom'), may hold values from -2 to 2
- levels: int32 [16, 6], P('grid'), may hold values from 0 to 7, as said below
- coefficients: int32 [16], P('grid'), may hold values from -3 to 3, as said below
Outputs:
- combined: float32 [16, 32, 4, 4, 8, 8, 128], P('grid', 'dom')
The draws below stay inside these ranges and needn't reach their ends.
Inputs may be any that keep to these rules, and one draw needn't show every extreme that they name: levels[g, k] is grid g's level along dimension k + 1. With L_k the base-two logarithm of that dimension's extent (32, 4, 4, 8, 8, 128), each entry lies between L_k - 2 and L_k, and the shortfalls L_k - levels[g, k] of one grid add up to 2 at most. `coefficients`: every coefficient is nonzero.
All inputs are finite; a program needn't handle non-finite values.
Results may differ from the reference program's by a relative error of at most 0.0003.
Values sent between devices are 32-bit elements; how exact they have to be, the bound alone decides.
No kernel may reach another device: no remote copies, remote signals or barrier semaphores. Data moves between devices by JAX's collectives and lax.ppermute only.
A program may use at most 64 MiB of HBM per device.

```python
import jax
import jax.numpy as jnp
import numpy as np
from jax import lax

EXT_B = 4
EXT_C = 4
EXT_D = 8
EXT_E = 8
EXT_F = 128
EXT_A = 32
GROUPS = 16


def draw_levels(key, part):
    picks = jax.random.randint(jax.random.fold_in(key, 11), (GROUPS, 2), 0, 7)
    doubled = jax.random.randint(jax.random.fold_in(key, 13), (), 0, GROUPS)
    single = jax.random.randint(jax.random.fold_in(key, 17), (), 0, GROUPS)
    picks = picks.at[single, 0].set(0)
    picks = picks.at[doubled].set(0)
    tops = jnp.array([EXT_A.bit_length() - 1, EXT_B.bit_length() - 1, EXT_C.bit_length() - 1, EXT_D.bit_length() - 1, EXT_E.bit_length() - 1, EXT_F.bit_length() - 1], dtype=jnp.int32)
    dims = jnp.arange(0, 6, dtype=jnp.int32)
    shortfall = jnp.sum((picks[:, :, None] == dims[None, None, :]).astype(jnp.int32), axis=1)
    return (tops[None, :] - shortfall).astype(jnp.int32)


def draw_coefficients(key, part):
    magnitude = jax.random.randint(jax.random.fold_in(key, 23), (GROUPS,), 1, 4)
    signs = jax.random.randint(jax.random.fold_in(key, 29), (GROUPS,), 0, 2) * 2 - 1
    return (magnitude * signs).astype(jnp.int32)


def shard_levels(key, shape, pieces, least, largest):
    def one(axis_at, parts):
        draws = jax.random.uniform(jax.random.fold_in(jax.random.fold_in(key, 6), axis_at), (parts,), jnp.float32, least / len(pieces), largest / len(pieces))
        return jnp.repeat(jnp.exp(draws), shape[axis_at] // parts).reshape((-1,) + (1,) * (len(shape) - axis_at - 1))

    gain = one(*pieces[0])
    for cut in pieces[1:]:
        gain = gain * one(*cut)
    return gain


def gaussian(rng, extent, width, bound, pieces=(), kind=jnp.bfloat16):
    drawn = width * jax.random.normal(rng, extent, jnp.float32)
    if pieces:
        drawn = drawn * shard_levels(rng, extent, pieces, -0.22, 0.18)
    return jnp.clip(drawn, -bound, bound).astype(kind)


def setup_inputs(seed: int = 0) -> dict:
    key_list = jax.random.split(jax.random.key(seed), 4)
    return {
        "values": gaussian(key_list[0], (GROUPS, EXT_A, EXT_B, EXT_C, EXT_D, EXT_E, EXT_F), 0.3, 2.0, ((0, 16), (1, 8)), jnp.float32),
        "levels": draw_levels(jax.random.fold_in(key_list[3], 71), 0),
        "coefficients": draw_coefficients(jax.random.fold_in(key_list[3], 71), 0),
    }


PRECISE = lax.Precision.HIGHEST


def coarse_position(numerator, level_now):
    while numerator > 0 and numerator % 2 == 0:
        numerator = numerator // 2
        level_now = level_now - 1
    if numerator == 0:
        return 0
    return (1 << (level_now - 1)) + (numerator - 1) // 2


def parent_positions(position):
    level_now = position.bit_length()
    span_size = 1 << (level_now - 1)
    offset = position - span_size
    return [coarse_position(offset % span_size, level_now - 1), coarse_position((offset + 1) % span_size, level_now - 1)]


def hier_table(points):
    matrix = np.eye(points)
    for position in range(1, points):
        for parent in parent_positions(position):
            matrix[position, parent] -= 0.5
    return matrix


def dehier_table(points):
    matrix = np.zeros((points, points))
    matrix[0, 0] = 1.0
    for position in range(1, points):
        row_now = np.zeros(points)
        row_now[position] = 1.0
        for parent in parent_positions(position):
            row_now = row_now + 0.5 * matrix[parent]
        matrix[position] = row_now
    return matrix


def nodal_order(points):
    placed = np.zeros(points, dtype=np.int64)
    for position in range(1, points):
        level_now = position.bit_length()
        offset = position - (1 << (level_now - 1))
        placed[position] = (2 * offset + 1) * points // (1 << level_now)
    return placed


def nodal_table(matrix):
    placed = nodal_order(matrix.shape[0])
    result = np.zeros(matrix.shape)
    result[placed[:, None], placed[None, :]] = matrix
    return result


def apply_table(grid_data, matrix, dim_index):
    letters = "abcdefg"[:grid_data.ndim]
    outputs = letters[:dim_index] + "z" + letters[dim_index + 1:]
    formula = letters + ",z" + letters[dim_index] + "->" + outputs
    return jnp.einsum(formula, grid_data, jnp.asarray(matrix, dtype=jnp.float32), precision=PRECISE)


def holding_mask(level_row, extents):
    holding = jnp.ones(extents, dtype=jnp.float32)
    for dim_index, points in enumerate(extents):
        count = level_row[dim_index].astype(jnp.int32)
        index = jnp.arange(points, dtype=jnp.int32)
        if dim_index == 0:
            spacing = jnp.right_shift(jnp.int32(points), count)
            inside = (jnp.remainder(index, spacing) == 0).astype(jnp.float32)
        else:
            limit = jnp.left_shift(jnp.int32(1), count)
            inside = (index < limit).astype(jnp.float32)
        shape_now = [1] * len(extents)
        shape_now[dim_index] = points
        holding = holding * inside.reshape(shape_now)
    return holding


def reference(values, levels, coefficients):
    extents = tuple(values.shape[1:])
    forward = [nodal_table(hier_table(values.shape[1]))] + [hier_table(points) for points in extents[1:]]
    backward = [nodal_table(dehier_table(values.shape[1]))] + [dehier_table(points) for points in extents[1:]]

    def accumulate(summed, scan_item):
        grid_data, level_row, weight = scan_item
        for dim_index, matrix in enumerate(forward):
            grid_data = apply_table(grid_data, matrix, dim_index)
        weighted = (weight.astype(jnp.float32) * holding_mask(level_row, extents)) * grid_data
        return summed + weighted, None

    initial = jnp.zeros(extents, dtype=jnp.float32)
    summed, unused = lax.scan(accumulate, initial, (values, levels, coefficients))
    combined = summed
    for dim_index, matrix in enumerate(backward):
        combined = apply_table(combined, matrix, dim_index)

    def restrict(level_row):
        return holding_mask(level_row, extents) * combined

    return lax.map(restrict, levels)
```

```python
import functools

import jax
import jax.numpy as jnp
import numpy as np
from jax import lax
from jax.experimental import pallas as pl
from jax.experimental.pallas import tpu as pltpu
from jax.sharding import PartitionSpec as P


TOPS = (5, 2, 2, 3, 3, 7)


def coarse_position(numerator, level_now):
    while numerator > 0 and numerator % 2 == 0:
        numerator = numerator // 2
        level_now = level_now - 1
    if numerator == 0:
        return 0
    return (1 << (level_now - 1)) + (numerator - 1) // 2


def parent_positions(position):
    level_now = position.bit_length()
    span_size = 1 << (level_now - 1)
    offset = position - span_size
    return [
        coarse_position(offset % span_size, level_now - 1),
        coarse_position((offset + 1) % span_size, level_now - 1),
    ]


def interp_tables(top):
    points = 1 << top
    result = []
    for short in range(3):
        matrix = np.eye(points)
        for position in range(points >> short, points):
            first, second = parent_positions(position)
            matrix[position] = 0.5 * (matrix[first] + matrix[second])
        result.append(matrix)
    return np.stack(result)


def two_sources(tables):
    sources = np.zeros((2, *tables.shape[:2]), dtype=np.int32)
    weights = np.zeros((2, *tables.shape[:2]), dtype=np.float32)
    for short in range(tables.shape[0]):
        for row in range(tables.shape[1]):
            found = np.nonzero(tables[short, row])[0]
            for i in range(2):
                at = found[min(i, len(found) - 1)]
                sources[i, short, row] = at
                weights[i, short, row] = tables[short, row, at] if i < len(found) else 0.0
    return sources, weights


def lead_interp(values, top, short):
    result = list(values)
    points = 1 << top
    for missing in (2, 1):
        for position in range(points >> missing, points >> (missing - 1)):
            first, second = parent_positions(position)
            if first == second:
                mean = result[first]
            else:
                mean = 0.5 * (result[first] + result[second])
            result[position] = jnp.where(short >= missing, mean, result[position])
    return result


def interp_kernel(levels, coefs, x, pf, src, wts, keep, send):
    core = lax.rem(lax.axis_index("grid"), 2)
    weight = coefs[0].astype(jnp.float32)
    short = [TOPS[k] - levels[0, k] for k in range(6)]
    matrix = pf[short[5]]
    rows = x[0, 0].reshape(1024, 128)
    high = rows.astype(jnp.bfloat16)
    low = (rows - high.astype(jnp.float32)).astype(jnp.bfloat16)
    along_f = jnp.dot(high, matrix, preferred_element_type=jnp.float32) + jnp.dot(
        low, matrix, preferred_element_type=jnp.float32
    )
    tiles = along_f.reshape(16, 8, 8, 128)
    src1, src2 = src[0, short[4]], src[1, short[4]]
    wt1, wt2 = wts[0, short[4]] * weight, wts[1, short[4]] * weight
    done = []
    for bc in range(16):
        along_e = []
        for d in range(8):
            tile = tiles[bc, d]
            along_e.append(
                wt1 * jnp.take_along_axis(tile, src1, axis=0) + wt2 * jnp.take_along_axis(tile, src2, axis=0)
            )
        done.append(lead_interp(along_e, 3, short[3]))
    for d in range(8):
        grid_now = [[done[b * 4 + c][d] for c in range(4)] for b in range(4)]
        grid_now = [lead_interp(line, 2, short[2]) for line in grid_now]
        columns = [lead_interp([grid_now[b][c] for b in range(4)], 2, short[1]) for c in range(4)]
        for b in range(4):
            for half in range(2):
                even, odd = columns[2 * half][b], columns[2 * half + 1][b]
                at = b * 2 + half
                keep[at, 0, d] = jnp.where(core == 0, even, odd)
                send[at, 0, d] = jnp.where(core == 0, odd, even)


def interp_rows(values, levels, coefs, tables, first, count):
    smem = pl.BlockSpec(memory_space=pltpu.SMEM)
    half = jax.ShapeDtypeStruct((8, count, 8, 8, 128), jnp.float32)
    out_spec = pl.BlockSpec((8, 1, 8, 8, 128), lambda a: (0, a, 0, 0, 0))
    return pl.pallas_call(
        interp_kernel,
        grid=(count,),
        in_specs=[
            smem,
            smem,
            pl.BlockSpec((1, 1, 4, 4, 8, 8, 128), lambda a: (0, a + first, 0, 0, 0, 0, 0)),
            pl.BlockSpec((3, 128, 128), lambda a: (0, 0, 0)),
            pl.BlockSpec((2, 3, 8, 128), lambda a: (0, 0, 0, 0)),
            pl.BlockSpec((2, 3, 8, 128), lambda a: (0, 0, 0, 0)),
        ],
        out_specs=[out_spec, out_spec],
        out_shape=[half, half],
        name=f"interp{count}",
    )(levels, coefs, values, *tables)


def combine_kernel(levels, others, own0, own123, got0, got123, next_own, next_got, out):
    short = TOPS[0] - levels[0, 0]
    other_short = TOPS[0] - others[0, 0]
    for at in range(2):
        for d in range(8):
            total = None
            for zero, rest, after, miss in (
                (own0, own123, next_own, short),
                (got0, got123, next_got, other_short),
            ):
                start, end = zero[at, 0, d], after[at, 0, d]
                one, two, three = (rest[at, i, d] for i in range(3))
                two = jnp.where(miss >= 2, 0.5 * (start + end), two)
                one = jnp.where(miss >= 1, 0.5 * (start + two), one)
                three = jnp.where(miss >= 1, 0.5 * (two + end), three)
                part = (start, one, two, three)
                total = part if total is None else tuple(s + t for s, t in zip(total, part))
            for i in range(4):
                out[at, i, d] = total[i]


def combine(levels, others, *pieces):
    smem = pl.BlockSpec(memory_space=pltpu.SMEM)
    specs = [pl.BlockSpec((2, p.shape[1], 8, 8, 128), lambda i: (i, 0, 0, 0, 0)) for p in pieces]
    return pl.pallas_call(
        combine_kernel,
        grid=(4,),
        in_specs=[smem, smem, *specs],
        out_specs=pl.BlockSpec((2, 4, 8, 8, 128), lambda i: (i, 0, 0, 0, 0)),
        out_shape=jax.ShapeDtypeStruct((8, 4, 8, 8, 128), jnp.float32),
        name="combine",
    )(levels, others, *pieces)


def restrict_kernel(levels, *refs):
    pieces, out = refs[:-1], refs[-1]
    index = lax.axis_index("grid")
    row = pl.program_id(0)
    short = [TOPS[k] - levels[0, k] for k in range(6)]
    point = lax.axis_index("dom") * 4 + row
    spacing = jnp.left_shift(jnp.int32(1), short[0])
    held_a = jnp.where(lax.rem(point, spacing) == 0, 1.0, 0.0)
    sublane = lax.broadcasted_iota(jnp.int32, (8, 128), 0)
    lane = lax.broadcasted_iota(jnp.int32, (8, 128), 1)
    tile = jnp.where(
        (sublane < jnp.right_shift(8, short[4])) & (lane < jnp.right_shift(128, short[5])), held_a, 0.0
    )
    by_d = [jnp.where(d < jnp.right_shift(8, short[3]), tile, 0.0) for d in range(8)]
    for slot, piece in enumerate(pieces):
        at = index ^ slot
        b, c = jnp.right_shift(at, 2), at & 3
        held = jnp.where(
            (b < jnp.right_shift(4, short[1])) & (c < jnp.right_shift(4, short[2])), 1.0, 0.0
        )
        for d in range(8):
            out[0, 0, b, c, d] = piece[0, d] * (by_d[d] * held)


def restrict(levels, pieces):
    smem = pl.BlockSpec(memory_space=pltpu.SMEM)
    return pl.pallas_call(
        restrict_kernel,
        grid=(4,),
        in_specs=[smem] + [pl.BlockSpec((1, 8, 8, 128), lambda a: (a, 0, 0, 0))] * 16,
        out_specs=pl.BlockSpec((1, 1, 4, 4, 8, 8, 128), lambda a: (0, a, 0, 0, 0, 0, 0)),
        out_shape=jax.ShapeDtypeStruct((1, 4, 4, 4, 8, 8, 128), jnp.float32),
        name="restrict",
    )(levels, *pieces)


def swap(x, bits):
    return lax.ppermute(x, "grid", [(i, i ^ bits) for i in range(16)])


def to_previous(x, bits):
    pairs = [(r * 8 + d, (r ^ bits) * 8 + (d - 1) % 8) for r in range(16) for d in range(8)]
    return lax.ppermute(x, ("grid", "dom"), pairs)


def body(values, levels, coefficients):
    src, wts = two_sources(interp_tables(3))
    tables = (
        jnp.asarray(interp_tables(7).transpose(0, 2, 1), dtype=jnp.bfloat16),
        jnp.asarray(np.broadcast_to(src[..., None], (2, 3, 8, 128))),
        jnp.asarray(np.broadcast_to(wts[..., None], (2, 3, 8, 128))),
    )
    others = swap(levels, 1)
    keep0, send0 = interp_rows(values, levels, coefficients, tables, 0, 1)
    next_own = to_previous(keep0, 0)
    next_got = to_previous(send0, 1)
    keep123, send123 = interp_rows(values, levels, coefficients, tables, 1, 3)
    got0, got123 = swap(send0, 1), swap(send123, 1)
    parts = combine(levels, others, keep0, keep123, got0, got123, next_own, next_got)
    groups = [[h * 2 + core for h in range(8)] for core in range(2)]
    arrived = lax.all_to_all(parts, "grid", split_axis=0, concat_axis=0, axis_index_groups=groups, tiled=True)
    share = arrived.sum(axis=0)
    pieces = {0: share}
    for bits in (4, 12, 2, 6, 14, 8, 10):
        pieces[bits] = swap(share, bits)
    for bits in list(pieces):
        pieces[bits + 1] = swap(pieces[bits], 1)
    return restrict(levels, [pieces[slot] for slot in range(16)])


def solution(mesh):
    in_specs = (P("grid", "dom", None, None, None, None, None), P("grid", None), P("grid"))
    out_specs = P("grid", "dom", None, None, None, None, None)
    return jax.shard_map(body, mesh=mesh, in_specs=in_specs, out_specs=out_specs, check_vma=False)
```

```python
import functools

import jax
import jax.numpy as jnp
import numpy as np
from jax import lax
from jax.experimental import pallas as pl
from jax.experimental.pallas import tpu as pltpu
from jax.sharding import PartitionSpec as P


TOPS = (5, 2, 2, 3, 3, 7)


def coarse_position(numerator, level_now):
    while numerator > 0 and numerator % 2 == 0:
        numerator = numerator // 2
        level_now = level_now - 1
    if numerator == 0:
        return 0
    return (1 << (level_now - 1)) + (numerator - 1) // 2


def parent_positions(position):
    level_now = position.bit_length()
    span_size = 1 << (level_now - 1)
    offset = position - span_size
    return [
        coarse_position(offset % span_size, level_now - 1),
        coarse_position((offset + 1) % span_size, level_now - 1),
    ]


def interp_tables(top):
    points = 1 << top
    result = []
    for short in range(3):
        matrix = np.eye(points)
        for position in range(points >> short, points):
            first, second = parent_positions(position)
            matrix[position] = 0.5 * (matrix[first] + matrix[second])
        result.append(matrix)
    return np.stack(result)


def two_sources(tables):
    sources = np.zeros((2, *tables.shape[:2]), dtype=np.int32)
    weights = np.zeros((2, *tables.shape[:2]), dtype=np.float32)
    for short in range(tables.shape[0]):
        for row in range(tables.shape[1]):
            found = np.nonzero(tables[short, row])[0]
            for i in range(2):
                at = found[min(i, len(found) - 1)]
                sources[i, short, row] = at
                weights[i, short, row] = tables[short, row, at] if i < len(found) else 0.0
    return sources, weights


def by_shortfall(table, short):
    sublane = lax.broadcasted_iota(jnp.int32, (8, 128), 0)
    kind = np.asarray(table).dtype.type
    result = jnp.full((8, 128), kind(0))
    for row in range(8):
        per = [kind(table[i, row]) for i in range(3)]
        here = jnp.where(short == 0, per[0], jnp.where(short == 1, per[1], per[2]))
        result = jnp.where(sublane == row, here, result)
    return result


def lead_interp(values, top, short):
    result = list(values)
    points = 1 << top
    for missing in (2, 1):
        for position in range(points >> missing, points >> (missing - 1)):
            first, second = parent_positions(position)
            if first == second:
                mean = result[first]
            else:
                mean = 0.5 * (result[first] + result[second])
            result[position] = jnp.where(short >= missing, mean, result[position])
    return result


def interp_kernel(levels, coefs, x, pf, *rest):
    keep, send = rest[-2:]
    core = lax.rem(lax.axis_index("grid"), 2)
    weight = coefs[0].astype(jnp.float32)
    short = [TOPS[k] - levels[0, k] for k in range(6)]
    matrix = pf[short[5]]
    rows = x[0, 0].reshape(1024, 128)
    high = rows.astype(jnp.bfloat16)
    low = (rows - high.astype(jnp.float32)).astype(jnp.bfloat16)
    along_f = jnp.dot(high, matrix, preferred_element_type=jnp.float32) + jnp.dot(
        low, matrix, preferred_element_type=jnp.float32
    )
    tiles = along_f.reshape(16, 8, 8, 128)
    sources, weights = two_sources(interp_tables(3))
    src1, src2 = (by_shortfall(sources[i], short[4]) for i in range(2))
    wt1, wt2 = (by_shortfall(weights[i], short[4]) * weight for i in range(2))
    done = []
    for bc in range(16):
        along_e = []
        for d in range(8):
            tile = tiles[bc, d]
            along_e.append(
                wt1 * jnp.take_along_axis(tile, src1, axis=0) + wt2 * jnp.take_along_axis(tile, src2, axis=0)
            )
        done.append(lead_interp(along_e, 3, short[3]))
    for d in range(8):
        grid_now = [[done[b * 4 + c][d] for c in range(4)] for b in range(4)]
        grid_now = [lead_interp(line, 2, short[2]) for line in grid_now]
        columns = [lead_interp([grid_now[b][c] for b in range(4)], 2, short[1]) for c in range(4)]
        for b in range(4):
            for half in range(2):
                even, odd = columns[2 * half][b], columns[2 * half + 1][b]
                at = b * 2 + half
                keep[at, 0, d] = jnp.where(core == 0, even, odd)
                send[at, 0, d] = jnp.where(core == 0, odd, even)


def in_vmem(x):
    return pltpu.with_memory_space_constraint(x, pltpu.VMEM)


def interp_rows(values, levels, coefs, matrices, first, count, after=()):
    smem = pl.BlockSpec(memory_space=pltpu.SMEM)
    half = jax.ShapeDtypeStruct((8, count, 8, 8, 128), jnp.float32)
    out_spec = pl.BlockSpec((8, 1, 8, 8, 128), lambda a: (0, a, 0, 0, 0))
    return pl.pallas_call(
        interp_kernel,
        grid=(count,),
        in_specs=[
            smem,
            smem,
            pl.BlockSpec((1, 1, 4, 4, 8, 8, 128), lambda a: (0, a + first, 0, 0, 0, 0, 0)),
            pl.BlockSpec((3, 128, 128), lambda a: (0, 0, 0)),
            *[pl.BlockSpec(memory_space=pl.ANY) for _ in after],
        ],
        out_specs=[out_spec, out_spec],
        out_shape=[half, half],
        compiler_params=pltpu.CompilerParams(vmem_limit_bytes=16 << 20),
        name=f"interp{count}",
    )(levels, coefs, pltpu.with_memory_space_constraint(values, pltpu.HBM), matrices, *after)


def combine_kernel(levels, others, own0, own123, got0, got123, next_own, next_got, out):
    short = TOPS[0] - levels[0, 0]
    other_short = TOPS[0] - others[0, 0]
    for at in range(8):
        for d in range(8):
            total = None
            for zero, rest, after, miss in (
                (own0, own123, next_own, short),
                (got0, got123, next_got, other_short),
            ):
                start, end = zero[at, 0, d], after[at, 0, d]
                one, two, three = (rest[at, i, d] for i in range(3))
                two = jnp.where(miss >= 2, 0.5 * (start + end), two)
                one = jnp.where(miss >= 1, 0.5 * (start + two), one)
                three = jnp.where(miss >= 1, 0.5 * (two + end), three)
                part = (start, one, two, three)
                total = part if total is None else tuple(s + t for s, t in zip(total, part))
            for i in range(4):
                out[at, i, d] = total[i]


def combine(levels, others, *pieces):
    smem = pl.BlockSpec(memory_space=pltpu.SMEM)
    vmem = pl.BlockSpec(memory_space=pltpu.VMEM)
    return pl.pallas_call(
        combine_kernel,
        in_specs=[smem, smem, *[vmem] * len(pieces)],
        out_specs=vmem,
        out_shape=pltpu.VMEM((8, 4, 8, 8, 128), jnp.float32),
        compiler_params=pltpu.CompilerParams(vmem_limit_bytes=4 << 20),
        name="combine",
    )(levels, others, *[in_vmem(p) for p in pieces])


def restrict_kernel(levels, *refs):
    pieces, out, scratch, sems = refs[:16], *refs[16:]
    index = lax.axis_index("grid")
    short = [TOPS[k] - levels[0, k] for k in range(6)]
    spacing = jnp.left_shift(jnp.int32(1), short[0])
    sublane = lax.broadcasted_iota(jnp.int32, (8, 128), 0)
    lane = lax.broadcasted_iota(jnp.int32, (8, 128), 1)
    inside = (sublane < jnp.right_shift(8, short[4])) & (lane < jnp.right_shift(128, short[5]))
    tile = jnp.where(inside, 1.0, 0.0)
    by_d = [jnp.where(d < jnp.right_shift(8, short[3]), tile, 0.0) for d in range(8)]
    copies = []
    for row in range(4):
        held_a = jnp.where(lax.rem(jnp.int32(row), spacing) == 0, 1.0, 0.0)
        for slot, piece in enumerate(pieces):
            at = index ^ slot
            b, c = jnp.right_shift(at, 2), at & 3
            held = jnp.where(
                (b < jnp.right_shift(4, short[1])) & (c < jnp.right_shift(4, short[2])), held_a, 0.0
            )
            for d in range(8):
                scratch[row, at, d] = piece[row, d] * (by_d[d] * held)
        copies.append(pltpu.make_async_copy(scratch.at[row], out.at[row], sems.at[row]))
        copies[-1].start()
    for copy in copies:
        copy.wait()


def restrict(levels, pieces):
    out = pl.pallas_call(
        restrict_kernel,
        in_specs=[pl.BlockSpec(memory_space=pltpu.SMEM)] + [pl.BlockSpec(memory_space=pltpu.VMEM)] * 16,
        out_specs=pl.BlockSpec(memory_space=pl.ANY),
        out_shape=jax.ShapeDtypeStruct((4, 16, 8, 8, 128), jnp.float32),
        scratch_shapes=[pltpu.VMEM((4, 16, 8, 8, 128), jnp.float32), pltpu.SemaphoreType.DMA((4,))],
        compiler_params=pltpu.CompilerParams(vmem_limit_bytes=4 << 20),
        name="restrict",
    )(levels, *[in_vmem(p) for p in pieces])
    return out.reshape(1, 4, 4, 4, 8, 8, 128)


def swap(x, bits):
    return lax.ppermute(x, "grid", [(i, i ^ bits) for i in range(16)])


def to_previous(x, bits):
    pairs = [(r * 8 + d, (r ^ bits) * 8 + (d - 1) % 8) for r in range(16) for d in range(8)]
    return lax.ppermute(x, ("grid", "dom"), pairs)


def body(values, levels, coefficients):
    matrices = jnp.asarray(interp_tables(7).transpose(0, 2, 1), dtype=jnp.bfloat16)
    others = swap(levels, 1)
    keep0, send0 = interp_rows(values, levels, coefficients, matrices, 0, 1)
    next_own = to_previous(keep0, 0)
    next_got = to_previous(send0, 1)
    keep123, send123 = interp_rows(values, levels, coefficients, matrices, 1, 3, (keep0,))
    got0, got123 = swap(send0, 1), swap(send123, 1)
    parts = combine(levels, others, keep0, keep123, got0, got123, next_own, next_got)
    groups = [[h * 2 + core for h in range(8)] for core in range(2)]
    arrived = lax.all_to_all(parts, "grid", split_axis=0, concat_axis=0, axis_index_groups=groups, tiled=True)
    share = arrived.sum(axis=0)
    pieces = {0: share}
    for bits in (4, 12, 2, 6, 14, 8, 10):
        pieces[bits] = swap(share, bits)
    for bits in list(pieces):
        pieces[bits + 1] = swap(pieces[bits], 1)
    return restrict(levels, [pieces[slot] for slot in range(16)])


def solution(mesh):
    in_specs = (P("grid", "dom", None, None, None, None, None), P("grid", None), P("grid"))
    out_specs = P("grid", "dom", None, None, None, None, None)
    return jax.shard_map(body, mesh=mesh, in_specs=in_specs, out_specs=out_specs, check_vma=False)
```

```python
import jax
import jax.numpy as jnp
import numpy as np
from jax import lax
from jax.experimental import pallas as pl
from jax.experimental.pallas import tpu as pltpu
from jax.sharding import PartitionSpec as P


TOPS = (5, 2, 2, 3, 3, 7)


def coarse_position(numerator, level_now):
    while numerator > 0 and numerator % 2 == 0:
        numerator = numerator // 2
        level_now = level_now - 1
    if numerator == 0:
        return 0
    return (1 << (level_now - 1)) + (numerator - 1) // 2


def parent_positions(position):
    level_now = position.bit_length()
    span_size = 1 << (level_now - 1)
    offset = position - span_size
    return [
        coarse_position(offset % span_size, level_now - 1),
        coarse_position((offset + 1) % span_size, level_now - 1),
    ]


def interp_tables(top):
    points = 1 << top
    result = []
    for short in range(3):
        matrix = np.eye(points)
        for position in range(points >> short, points):
            first, second = parent_positions(position)
            matrix[position] = 0.5 * (matrix[first] + matrix[second])
        result.append(matrix)
    return np.stack(result)


def two_sources(tables):
    sources = np.zeros((2, *tables.shape[:2]), dtype=np.int32)
    weights = np.zeros((2, *tables.shape[:2]), dtype=np.float32)
    for short in range(tables.shape[0]):
        for row in range(tables.shape[1]):
            found = np.nonzero(tables[short, row])[0]
            for i in range(2):
                at = found[min(i, len(found) - 1)]
                sources[i, short, row] = at
                weights[i, short, row] = tables[short, row, at] if i < len(found) else 0.0
    return sources, weights


def by_shortfall(table, short):
    sublane = lax.broadcasted_iota(jnp.int32, (8, 128), 0)
    kind = np.asarray(table).dtype.type
    result = jnp.full((8, 128), kind(0))
    for row in range(8):
        per = [kind(table[i, row]) for i in range(3)]
        here = jnp.where(short == 0, per[0], jnp.where(short == 1, per[1], per[2]))
        result = jnp.where(sublane == row, here, result)
    return result


def lead_interp(values, top, short):
    result = list(values)
    points = 1 << top
    for missing in (2, 1):
        for position in range(points >> missing, points >> (missing - 1)):
            first, second = parent_positions(position)
            if first == second:
                mean = result[first]
            else:
                mean = 0.5 * (result[first] + result[second])
            result[position] = jnp.where(short >= missing, mean, result[position])
    return result


def interp_kernel(levels, coefs, x, pf, *rest):
    keep, send = rest[-2:]
    core = lax.rem(lax.axis_index("grid"), 2)
    weight = coefs[0].astype(jnp.float32)
    short = [TOPS[k] - levels[0, k] for k in range(6)]
    matrix = pf[short[5]]
    rows = x[0, 0].reshape(1024, 128)
    high = rows.astype(jnp.bfloat16)
    low = (rows - high.astype(jnp.float32)).astype(jnp.bfloat16)
    along_f = jnp.dot(high, matrix, preferred_element_type=jnp.float32) + jnp.dot(
        low, matrix, preferred_element_type=jnp.float32
    )
    tiles = along_f.reshape(16, 8, 8, 128)
    sources, weights = two_sources(interp_tables(3))
    src1, src2 = (by_shortfall(sources[i], short[4]) for i in range(2))
    wt1, wt2 = (by_shortfall(weights[i], short[4]) * weight for i in range(2))
    done = []
    for bc in range(16):
        along_e = []
        for d in range(8):
            tile = tiles[bc, d]
            along_e.append(
                wt1 * jnp.take_along_axis(tile, src1, axis=0) + wt2 * jnp.take_along_axis(tile, src2, axis=0)
            )
        done.append(lead_interp(along_e, 3, short[3]))
    for d in range(8):
        grid_now = [[done[b * 4 + c][d] for c in range(4)] for b in range(4)]
        grid_now = [lead_interp(line, 2, short[2]) for line in grid_now]
        columns = [lead_interp([grid_now[b][c] for b in range(4)], 2, short[1]) for c in range(4)]
        for b in range(4):
            for half in range(2):
                even, odd = columns[2 * half][b], columns[2 * half + 1][b]
                at = b * 2 + half
                keep[at, 0, d] = jnp.where(core == 0, even, odd)
                send[at, 0, d] = jnp.where(core == 0, odd, even)


def in_vmem(x):
    return pltpu.with_memory_space_constraint(x, pltpu.VMEM)


def in_hbm(x):
    return pltpu.with_memory_space_constraint(x, pltpu.HBM)


def interp_rows(values, levels, coefs, matrices, first, count, after=()):
    smem = pl.BlockSpec(memory_space=pltpu.SMEM)
    half = jax.ShapeDtypeStruct((8, count, 8, 8, 128), jnp.float32)
    out_spec = pl.BlockSpec((8, 1, 8, 8, 128), lambda a: (0, a, 0, 0, 0))
    return pl.pallas_call(
        interp_kernel,
        grid=(count,),
        in_specs=[
            smem,
            smem,
            pl.BlockSpec((1, 1, 4, 4, 8, 8, 128), lambda a: (0, a + first, 0, 0, 0, 0, 0)),
            pl.BlockSpec((3, 128, 128), lambda a: (0, 0, 0)),
            *[pl.BlockSpec(memory_space=pl.ANY) for _ in after],
        ],
        out_specs=[out_spec, out_spec],
        out_shape=[half, half],
        compiler_params=pltpu.CompilerParams(vmem_limit_bytes=16 << 20),
        cost_estimate=pl.CostEstimate(flops=count * 10**8, bytes_accessed=count << 20, transcendentals=0),
    )(in_hbm(levels), coefs, in_hbm(values), in_hbm(matrices), *after)


def combine_kernel(levels, others, own0, own123, got0, got123, next_own, next_got, out):
    short = TOPS[0] - levels[0, 0]
    other_short = TOPS[0] - others[0, 0]
    for at in range(8):
        for d in range(8):
            total = None
            for zero, rest, after, miss in (
                (own0, own123, next_own, short),
                (got0, got123, next_got, other_short),
            ):
                start, end = zero[at, 0, d], after[at, 0, d]
                one, two, three = (rest[at, i, d] for i in range(3))
                two = jnp.where(miss >= 2, 0.5 * (start + end), two)
                one = jnp.where(miss >= 1, 0.5 * (start + two), one)
                three = jnp.where(miss >= 1, 0.5 * (two + end), three)
                part = (start, one, two, three)
                total = part if total is None else tuple(s + t for s, t in zip(total, part))
            for i in range(4):
                out[at, i, d] = total[i]


def combine(levels, others, *pieces):
    smem = pl.BlockSpec(memory_space=pltpu.SMEM)
    vmem = pl.BlockSpec(memory_space=pltpu.VMEM)
    return pl.pallas_call(
        combine_kernel,
        in_specs=[smem, smem, *[vmem] * len(pieces)],
        out_specs=vmem,
        out_shape=pltpu.VMEM((8, 4, 8, 8, 128), jnp.float32),
        compiler_params=pltpu.CompilerParams(vmem_limit_bytes=4 << 20),
        name="combine",
    )(levels, others, *[in_vmem(p) for p in pieces])


def restrict_kernel(levels, *refs):
    pieces, out, scratch, sems = refs[:16], *refs[16:]
    index = lax.axis_index("grid")
    short = [TOPS[k] - levels[0, k] for k in range(6)]
    spacing = jnp.left_shift(jnp.int32(1), short[0])
    sublane = lax.broadcasted_iota(jnp.int32, (8, 128), 0)
    lane = lax.broadcasted_iota(jnp.int32, (8, 128), 1)
    inside = (sublane < jnp.right_shift(8, short[4])) & (lane < jnp.right_shift(128, short[5]))
    tile = jnp.where(inside, 1.0, 0.0)
    by_d = [jnp.where(d < jnp.right_shift(8, short[3]), tile, 0.0) for d in range(8)]
    copies = []
    for row in range(4):
        held_a = jnp.where(lax.rem(jnp.int32(row), spacing) == 0, 1.0, 0.0)
        for slot, piece in enumerate(pieces):
            at = index ^ slot
            b, c = jnp.right_shift(at, 2), at & 3
            held = jnp.where(
                (b < jnp.right_shift(4, short[1])) & (c < jnp.right_shift(4, short[2])), held_a, 0.0
            )
            for d in range(8):
                scratch[row, at, d] = piece[row, d] * (by_d[d] * held)
        copies.append(pltpu.make_async_copy(scratch.at[row], out.at[row], sems.at[row]))
        copies[-1].start()
    for copy in copies:
        copy.wait()


def restrict(levels, pieces):
    out = pl.pallas_call(
        restrict_kernel,
        in_specs=[pl.BlockSpec(memory_space=pltpu.SMEM)] + [pl.BlockSpec(memory_space=pltpu.VMEM)] * 16,
        out_specs=pl.BlockSpec(memory_space=pl.ANY),
        out_shape=jax.ShapeDtypeStruct((4, 16, 8, 8, 128), jnp.float32),
        scratch_shapes=[pltpu.VMEM((4, 16, 8, 8, 128), jnp.float32), pltpu.SemaphoreType.DMA((4,))],
        compiler_params=pltpu.CompilerParams(vmem_limit_bytes=4 << 20),
        name="restrict",
    )(levels, *[in_vmem(p) for p in pieces])
    return out.reshape(1, 4, 4, 4, 8, 8, 128)


def swap(x, bits):
    return lax.ppermute(x, "grid", [(i, i ^ bits) for i in range(16)])


def to_previous(x, bits):
    pairs = [(r * 8 + d, (r ^ bits) * 8 + (d - 1) % 8) for r in range(16) for d in range(8)]
    return lax.ppermute(x, ("grid", "dom"), pairs)


def whole(values, levels, coefficients):
    matrices = jnp.asarray(interp_tables(7).transpose(0, 2, 1), dtype=jnp.bfloat16)
    others = swap(levels, 1)
    keep0, send0 = interp_rows(values, levels, coefficients, matrices, 0, 1)
    next_own = to_previous(keep0, 0)
    next_got = to_previous(send0, 1)
    keep123, send123 = interp_rows(values, levels, coefficients, matrices, 1, 3, (keep0,))
    got0, got123 = swap(send0, 1), swap(send123, 1)
    parts = combine(levels, others, keep0, keep123, got0, got123, next_own, next_got)
    groups = [[h * 2 + core for h in range(8)] for core in range(2)]
    arrived = lax.all_to_all(parts, "grid", split_axis=0, concat_axis=0, axis_index_groups=groups, tiled=True)
    share = arrived.sum(axis=0)
    pieces = {0: share}
    for bits in (4, 12, 2, 6, 14, 8, 10):
        pieces[bits] = swap(share, bits)
    for bits in list(pieces):
        pieces[bits + 1] = swap(pieces[bits], 1)
    return restrict(levels, [pieces[slot] for slot in range(16)])


def solution(mesh):
    in_specs = (P("grid", "dom", None, None, None, None, None), P("grid", None), P("grid"))
    out_specs = P("grid", "dom", None, None, None, None, None)
    return jax.shard_map(whole, mesh=mesh, in_specs=in_specs, out_specs=out_specs, check_vma=False)
```

```python
import jax
import jax.numpy as jnp
import numpy as np
from jax import lax
from jax.experimental import pallas as pl
from jax.experimental.pallas import tpu as pltpu
from jax.sharding import PartitionSpec as P


TOPS = (5, 2, 2, 3, 3, 7)


def coarse_position(numerator, level_now):
    while numerator > 0 and numerator % 2 == 0:
        numerator = numerator // 2
        level_now = level_now - 1
    if numerator == 0:
        return 0
    return (1 << (level_now - 1)) + (numerator - 1) // 2


def parent_positions(position):
    level_now = position.bit_length()
    span_size = 1 << (level_now - 1)
    offset = position - span_size
    return [
        coarse_position(offset % span_size, level_now - 1),
        coarse_position((offset + 1) % span_size, level_now - 1),
    ]


def interp_tables(top):
    points = 1 << top
    result = []
    for short in range(3):
        matrix = np.eye(points)
        for position in range(points >> short, points):
            first, second = parent_positions(position)
            matrix[position] = 0.5 * (matrix[first] + matrix[second])
        result.append(matrix)
    return np.stack(result)


def two_sources(tables):
    sources = np.zeros((2, *tables.shape[:2]), dtype=np.int32)
    weights = np.zeros((2, *tables.shape[:2]), dtype=np.float32)
    for short in range(tables.shape[0]):
        for row in range(tables.shape[1]):
            found = np.nonzero(tables[short, row])[0]
            for i in range(2):
                at = found[min(i, len(found) - 1)]
                sources[i, short, row] = at
                weights[i, short, row] = tables[short, row, at] if i < len(found) else 0.0
    return sources, weights


def by_shortfall(table, short):
    sublane = lax.broadcasted_iota(jnp.int32, (8, 128), 0)
    kind = np.asarray(table).dtype.type
    result = jnp.full((8, 128), kind(0))
    for row in range(8):
        per = [kind(table[i, row]) for i in range(3)]
        here = jnp.where(short == 0, per[0], jnp.where(short == 1, per[1], per[2]))
        result = jnp.where(sublane == row, here, result)
    return result


def lead_interp(values, top, short):
    result = list(values)
    points = 1 << top
    for missing in (2, 1):
        for position in range(points >> missing, points >> (missing - 1)):
            first, second = parent_positions(position)
            if first == second:
                mean = result[first]
            else:
                mean = 0.5 * (result[first] + result[second])
            result[position] = jnp.where(short >= missing, mean, result[position])
    return result


def interp_kernel(levels, coefs, x, pf, *rest):
    keep, send = rest[-2:]
    core = lax.rem(lax.axis_index("grid"), 2)
    weight = coefs[0].astype(jnp.float32)
    short = [TOPS[k] - levels[0, k] for k in range(6)]
    matrix = pf[short[5]]
    rows = x[0, 0].reshape(1024, 128)
    high = rows.astype(jnp.bfloat16)
    low = (rows - high.astype(jnp.float32)).astype(jnp.bfloat16)
    along_f = jnp.dot(high, matrix, preferred_element_type=jnp.float32) + jnp.dot(
        low, matrix, preferred_element_type=jnp.float32
    )
    tiles = along_f.reshape(16, 8, 8, 128)
    sources, weights = two_sources(interp_tables(3))
    src1, src2 = (by_shortfall(sources[i], short[4]) for i in range(2))
    wt1, wt2 = (by_shortfall(weights[i], short[4]) * weight for i in range(2))
    done = []
    for bc in range(16):
        along_e = []
        for d in range(8):
            tile = tiles[bc, d]
            along_e.append(
                wt1 * jnp.take_along_axis(tile, src1, axis=0) + wt2 * jnp.take_along_axis(tile, src2, axis=0)
            )
        done.append(lead_interp(along_e, 3, short[3]))
    for d in range(8):
        grid_now = [[done[b * 4 + c][d] for c in range(4)] for b in range(4)]
        grid_now = [lead_interp(line, 2, short[2]) for line in grid_now]
        columns = [lead_interp([grid_now[b][c] for b in range(4)], 2, short[1]) for c in range(4)]
        for b in range(4):
            for half in range(2):
                even, odd = columns[2 * half][b], columns[2 * half + 1][b]
                at = b * 2 + half
                keep[at, 0, d] = jnp.where(core == 0, even, odd)
                send[at, 0, d] = jnp.where(core == 0, odd, even)


def in_vmem(x):
    return pltpu.with_memory_space_constraint(x, pltpu.VMEM)


def in_hbm(x):
    return pltpu.with_memory_space_constraint(x, pltpu.HBM)


def interp_rows(values, levels, coefs, matrices, first, count, after=()):
    smem = pl.BlockSpec(memory_space=pltpu.SMEM)
    half = jax.ShapeDtypeStruct((8, count, 8, 8, 128), jnp.float32)
    out_spec = pl.BlockSpec((8, 1, 8, 8, 128), lambda a: (0, a, 0, 0, 0))
    return pl.pallas_call(
        interp_kernel,
        grid=(count,),
        in_specs=[
            smem,
            smem,
            pl.BlockSpec((1, 1, 4, 4, 8, 8, 128), lambda a: (0, a + first, 0, 0, 0, 0, 0)),
            pl.BlockSpec((3, 128, 128), lambda a: (0, 0, 0)),
            *[pl.BlockSpec(memory_space=pl.ANY) for _ in after],
        ],
        out_specs=[out_spec, out_spec],
        out_shape=[half, half],
        compiler_params=pltpu.CompilerParams(vmem_limit_bytes=16 << 20),
        cost_estimate=pl.CostEstimate(flops=count * 10**8, bytes_accessed=count << 20, transcendentals=0),
    )(in_hbm(levels), coefs, in_hbm(values), in_hbm(matrices), *after)


def combine_kernel(levels, others, own0, own123, got0, got123, next_own, next_got, out):
    short = TOPS[0] - levels[0, 0]
    other_short = TOPS[0] - others[0, 0]
    for at in range(8):
        for d in range(8):
            total = None
            for zero, rest, after, miss in (
                (own0, own123, next_own, short),
                (got0, got123, next_got, other_short),
            ):
                start, end = zero[at, 0, d], after[at, 0, d]
                one, two, three = (rest[at, i, d] for i in range(3))
                two = jnp.where(miss >= 2, 0.5 * (start + end), two)
                one = jnp.where(miss >= 1, 0.5 * (start + two), one)
                three = jnp.where(miss >= 1, 0.5 * (two + end), three)
                part = (start, one, two, three)
                total = part if total is None else tuple(s + t for s, t in zip(total, part))
            for i in range(4):
                out[at, i, d] = total[i]


def combine(levels, others, *pieces):
    smem = pl.BlockSpec(memory_space=pltpu.SMEM)
    vmem = pl.BlockSpec(memory_space=pltpu.VMEM)
    return pl.pallas_call(
        combine_kernel,
        in_specs=[smem, smem, *[vmem] * len(pieces)],
        out_specs=vmem,
        out_shape=pltpu.VMEM((8, 4, 8, 8, 128), jnp.float32),
        compiler_params=pltpu.CompilerParams(vmem_limit_bytes=4 << 20),
        name="combine",
    )(levels, others, *[in_vmem(p) for p in pieces])


def restrict_kernel(levels, *refs):
    pieces, out, scratch, sems = refs[:16], *refs[16:]
    index = lax.axis_index("grid")
    short = [TOPS[k] - levels[0, k] for k in range(6)]
    spacing = jnp.left_shift(jnp.int32(1), short[0])
    sublane = lax.broadcasted_iota(jnp.int32, (8, 128), 0)
    lane = lax.broadcasted_iota(jnp.int32, (8, 128), 1)
    inside = (sublane < jnp.right_shift(8, short[4])) & (lane < jnp.right_shift(128, short[5]))
    tile = jnp.where(inside, 1.0, 0.0)
    by_d = [jnp.where(d < jnp.right_shift(8, short[3]), tile, 0.0) for d in range(8)]
    copies = []
    for row in range(4):
        held_a = jnp.where(lax.rem(jnp.int32(row), spacing) == 0, 1.0, 0.0)
        for slot, piece in enumerate(pieces):
            at = index ^ slot
            b, c = jnp.right_shift(at, 2), at & 3
            held = jnp.where(
                (b < jnp.right_shift(4, short[1])) & (c < jnp.right_shift(4, short[2])), held_a, 0.0
            )
            for d in range(8):
                scratch[row, at, d] = piece[row, d] * (by_d[d] * held)
        copies.append(pltpu.make_async_copy(scratch.at[row], out.at[row], sems.at[row]))
        copies[-1].start()
    for copy in copies:
        copy.wait()


def restrict(levels, pieces):
    out = pl.pallas_call(
        restrict_kernel,
        in_specs=[pl.BlockSpec(memory_space=pltpu.SMEM)] + [pl.BlockSpec(memory_space=pltpu.VMEM)] * 16,
        out_specs=pl.BlockSpec(memory_space=pl.ANY),
        out_shape=jax.ShapeDtypeStruct((4, 16, 8, 8, 128), jnp.float32),
        scratch_shapes=[pltpu.VMEM((4, 16, 8, 8, 128), jnp.float32), pltpu.SemaphoreType.DMA((4,))],
        compiler_params=pltpu.CompilerParams(vmem_limit_bytes=4 << 20),
        name="restrict",
    )(levels, *[in_vmem(p) for p in pieces])
    return out.reshape(1, 4, 4, 4, 8, 8, 128)


def swap(x, bits):
    return lax.ppermute(x, "grid", [(i, i ^ bits) for i in range(16)])


def to_previous(x, bits):
    pairs = [(r * 8 + d, (r ^ bits) * 8 + (d - 1) % 8) for r in range(16) for d in range(8)]
    return lax.ppermute(x, ("grid", "dom"), pairs)


GATHER = ((2, 0), (8, 0), (4, 0), (12, 0), (4, 2), (12, 2), (2, 8))


def whole(values, levels, coefficients):
    matrices = jnp.asarray(interp_tables(7).transpose(0, 2, 1), dtype=jnp.bfloat16)
    others = swap(levels, 1)
    keep0, send0 = interp_rows(values, levels, coefficients, matrices, 0, 1)
    next_own = to_previous(keep0, 0)
    next_got = to_previous(send0, 1)
    keep123, send123 = interp_rows(values, levels, coefficients, matrices, 1, 3, (keep0,))
    got0, got123 = swap(send0, 1), swap(send123, 1)
    parts = combine(levels, others, keep0, keep123, got0, got123, next_own, next_got)
    groups = [[h * 2 + core for h in range(8)] for core in range(2)]
    arrived = lax.all_to_all(parts, "grid", split_axis=0, concat_axis=0, axis_index_groups=groups, tiled=True)
    share = arrived.sum(axis=0)
    pieces = {0: share}
    for bits, first in GATHER:
        pieces[bits ^ first] = swap(pieces[first], bits)
    for bits in list(pieces):
        pieces[bits + 1] = swap(pieces[bits], 1)
    return restrict(levels, [pieces[slot] for slot in range(16)])


def solution(mesh):
    in_specs = (P("grid", "dom", None, None, None, None, None), P("grid", None), P("grid"))
    out_specs = P("grid", "dom", None, None, None, None, None)
    return jax.shard_map(whole, mesh=mesh, in_specs=in_specs, out_specs=out_specs, check_vma=False)
```

```python
import jax
import jax.numpy as jnp
import numpy as np
from jax import lax
from jax.experimental import pallas as pl
from jax.experimental.pallas import tpu as pltpu
from jax.sharding import PartitionSpec as P


TOPS = (5, 2, 2, 3, 3, 7)
FIRST = (5, 3, 7, 4)
SECOND = (1, 2, 6, 0)


def coarse_position(numerator, level_now):
    while numerator > 0 and numerator % 2 == 0:
        numerator = numerator // 2
        level_now = level_now - 1
    if numerator == 0:
        return 0
    return (1 << (level_now - 1)) + (numerator - 1) // 2


def parent_positions(position):
    level_now = position.bit_length()
    span_size = 1 << (level_now - 1)
    offset = position - span_size
    return [
        coarse_position(offset % span_size, level_now - 1),
        coarse_position((offset + 1) % span_size, level_now - 1),
    ]


def interp_tables(top):
    points = 1 << top
    result = []
    for short in range(3):
        matrix = np.eye(points)
        for position in range(points >> short, points):
            first, second = parent_positions(position)
            matrix[position] = 0.5 * (matrix[first] + matrix[second])
        result.append(matrix)
    return np.stack(result)


def two_sources(tables):
    sources = np.zeros((2, *tables.shape[:2]), dtype=np.int32)
    weights = np.zeros((2, *tables.shape[:2]), dtype=np.float32)
    for short in range(tables.shape[0]):
        for row in range(tables.shape[1]):
            found = np.nonzero(tables[short, row])[0]
            for i in range(2):
                at = found[min(i, len(found) - 1)]
                sources[i, short, row] = at
                weights[i, short, row] = tables[short, row, at] if i < len(found) else 0.0
    return sources, weights


def by_shortfall(table, short):
    sublane = lax.broadcasted_iota(jnp.int32, (8, 128), 0)
    kind = np.asarray(table).dtype.type
    result = jnp.full((8, 128), kind(0))
    for row in range(8):
        per = [kind(table[i, row]) for i in range(3)]
        here = jnp.where(short == 0, per[0], jnp.where(short == 1, per[1], per[2]))
        result = jnp.where(sublane == row, here, result)
    return result


def lead_interp(values, top, short):
    result = list(values)
    points = 1 << top
    for missing in (2, 1):
        for position in range(points >> missing, points >> (missing - 1)):
            first, second = parent_positions(position)
            if first == second:
                mean = result[first]
            else:
                mean = 0.5 * (result[first] + result[second])
            result[position] = jnp.where(short >= missing, mean, result[position])
    return result


def interp_kernel(levels, coefs, x, pf, *rest):
    keep, send, done = rest[-3:]
    index = lax.axis_index("grid")
    here, core = jnp.right_shift(index, 1), index & 1
    weight = coefs[0].astype(jnp.float32)
    short = [TOPS[k] - levels[0, k] for k in range(6)]
    matrix = pf[short[5]]
    rows = x[0, 0].reshape(1024, 128)
    high = rows.astype(jnp.bfloat16)
    low = (rows - high.astype(jnp.float32)).astype(jnp.bfloat16)
    along_f = jnp.dot(high, matrix, preferred_element_type=jnp.float32) + jnp.dot(
        low, matrix, preferred_element_type=jnp.float32
    )
    tiles = along_f.reshape(16, 8, 8, 128)
    sources, weights = two_sources(interp_tables(3))
    src1, src2 = (by_shortfall(sources[i], short[4]) for i in range(2))
    wt1, wt2 = (by_shortfall(weights[i], short[4]) * weight for i in range(2))
    by_bc = []
    for bc in range(16):
        along_e = []
        for d in range(8):
            tile = tiles[bc, d]
            along_e.append(
                wt1 * jnp.take_along_axis(tile, src1, axis=0) + wt2 * jnp.take_along_axis(tile, src2, axis=0)
            )
        by_bc.append(lead_interp(along_e, 3, short[3]))
    for d in range(8):
        lines = [lead_interp([by_bc[b * 4 + c][d] for c in range(4)], 2, short[2]) for b in range(4)]
        for c in range(4):
            for b, value in enumerate(lead_interp([lines[b][c] for b in range(4)], 2, short[1])):
                done[b * 4 + c, d] = value
    for i in range(4):
        kept = jnp.where(core == 1, FIRST[i], SECOND[i]) ^ here
        sent = jnp.where(core == 1, SECOND[i], FIRST[i]) ^ here
        for c in range(2):
            for d in range(8):
                keep[i, 0, c, d] = done[kept * 2 + c, d]
                send[i, 0, c, d] = done[sent * 2 + c, d]


def in_vmem(x):
    return pltpu.with_memory_space_constraint(x, pltpu.VMEM)


def in_hbm(x):
    return pltpu.with_memory_space_constraint(x, pltpu.HBM)


def interp_rows(values, levels, coefs, matrices, first, count, after=()):
    smem = pl.BlockSpec(memory_space=pltpu.SMEM)
    half = jax.ShapeDtypeStruct((4, count, 2, 8, 8, 128), jnp.float32)
    out_spec = pl.BlockSpec((4, 1, 2, 8, 8, 128), lambda a: (0, a, 0, 0, 0, 0))
    return pl.pallas_call(
        interp_kernel,
        grid=(count,),
        in_specs=[
            smem,
            smem,
            pl.BlockSpec((1, 1, 4, 4, 8, 8, 128), lambda a: (0, a + first, 0, 0, 0, 0, 0)),
            pl.BlockSpec((3, 128, 128), lambda a: (0, 0, 0)),
            *[pl.BlockSpec(memory_space=pl.ANY) for _ in after],
        ],
        out_specs=[out_spec, out_spec],
        out_shape=[half, half],
        scratch_shapes=[pltpu.VMEM((16, 8, 8, 128), jnp.float32)],
        compiler_params=pltpu.CompilerParams(vmem_limit_bytes=16 << 20),
        cost_estimate=pl.CostEstimate(flops=count * 10**8, bytes_accessed=count << 20, transcendentals=0),
    )(in_hbm(levels), coefs, in_hbm(values), in_hbm(matrices), *after)


def combine_kernel(levels, others, own0, own123, got0, got123, next_own, next_got, *outs):
    short = TOPS[0] - levels[0, 0]
    other_short = TOPS[0] - others[0, 0]
    for at, out in enumerate(outs):
        for c in range(2):
            for d in range(8):
                total = None
                for zero, rest, after, miss in (
                    (own0, own123, next_own, short),
                    (got0, got123, next_got, other_short),
                ):
                    start, end = zero[at, 0, c, d], after[at, 0, c, d]
                    one, two, three = (rest[at, i, c, d] for i in range(3))
                    two = jnp.where(miss >= 2, 0.5 * (start + end), two)
                    one = jnp.where(miss >= 1, 0.5 * (start + two), one)
                    three = jnp.where(miss >= 1, 0.5 * (two + end), three)
                    part = (start, one, two, three)
                    total = part if total is None else tuple(s + t for s, t in zip(total, part))
                for i in range(4):
                    out[i, c, d] = total[i]


def combine(levels, others, *pieces):
    smem = pl.BlockSpec(memory_space=pltpu.SMEM)
    vmem = pl.BlockSpec(memory_space=pltpu.VMEM)
    return pl.pallas_call(
        combine_kernel,
        in_specs=[smem, smem, *[vmem] * len(pieces)],
        out_specs=[vmem] * 4,
        out_shape=[pltpu.VMEM((4, 2, 8, 8, 128), jnp.float32)] * 4,
        compiler_params=pltpu.CompilerParams(vmem_limit_bytes=4 << 20),
        name="combine",
    )(levels, others, *[in_vmem(p) for p in pieces])


def restrict_kernel(levels, *refs):
    north, south, out, scratch, sems = refs[:8], refs[8:16], *refs[16:]
    here = jnp.right_shift(lax.axis_index("grid"), 1)
    short = [TOPS[k] - levels[0, k] for k in range(6)]
    spacing = jnp.left_shift(jnp.int32(1), short[0])
    sublane = lax.broadcasted_iota(jnp.int32, (8, 128), 0)
    lane = lax.broadcasted_iota(jnp.int32, (8, 128), 1)
    inside = (sublane < jnp.right_shift(8, short[4])) & (lane < jnp.right_shift(128, short[5]))
    tile = jnp.where(inside, 1.0, 0.0)
    by_d = [jnp.where(d < jnp.right_shift(8, short[3]), tile, 0.0) for d in range(8)]
    copies = []
    for row in range(4):
        held_a = jnp.where(lax.rem(jnp.int32(row), spacing) == 0, 1.0, 0.0)
        for slot in range(8):
            for half in range(2):
                at = (here ^ slot) * 2 + half
                b, c = jnp.right_shift(at, 2), at & 3
                held = jnp.where(
                    (b < jnp.right_shift(4, short[1])) & (c < jnp.right_shift(4, short[2])), held_a, 0.0
                )
                for d in range(8):
                    value = north[slot][row, half, d] + south[slot][row, half, d]
                    scratch[row, at, d] = value * (by_d[d] * held)
        copies.append(pltpu.make_async_copy(scratch.at[row], out.at[row], sems.at[row]))
        copies[-1].start()
    for copy in copies:
        copy.wait()


def restrict(levels, pieces):
    out = pl.pallas_call(
        restrict_kernel,
        in_specs=[pl.BlockSpec(memory_space=pltpu.SMEM)] + [pl.BlockSpec(memory_space=pltpu.VMEM)] * 16,
        out_specs=pl.BlockSpec(memory_space=pl.ANY),
        out_shape=jax.ShapeDtypeStruct((4, 16, 8, 8, 128), jnp.float32),
        scratch_shapes=[pltpu.VMEM((4, 16, 8, 8, 128), jnp.float32), pltpu.SemaphoreType.DMA((4,))],
        compiler_params=pltpu.CompilerParams(vmem_limit_bytes=4 << 20),
        name="restrict",
    )(levels, *[in_vmem(p) for p in pieces])
    return out.reshape(1, 4, 4, 4, 8, 8, 128)


def swap(x, bits):
    return lax.ppermute(x, "grid", [(i, i ^ bits) for i in range(16)])


def between(x, bits, cores):
    return lax.ppermute(x, "grid", [(h * 2 + core, (h ^ bits) * 2 + core) for h in range(8) for core in cores])


def across(x, core):
    return lax.ppermute(x, "grid", [(h * 2 + core, h * 2 + 1 - core) for h in range(8)])


def to_previous(x, bits):
    pairs = [(r * 8 + d, (r ^ bits) * 8 + (d - 1) % 8) for r in range(16) for d in range(8)]
    return lax.ppermute(x, ("grid", "dom"), pairs)


def whole(values, levels, coefficients):
    matrices = jnp.asarray(interp_tables(7).transpose(0, 2, 1), dtype=jnp.bfloat16)
    others = swap(levels, 1)
    keep0, send0 = interp_rows(values, levels, coefficients, matrices, 0, 1)
    next_own = to_previous(keep0, 0)
    next_got = to_previous(send0, 1)
    keep123, send123 = interp_rows(values, levels, coefficients, matrices, 1, 3, (keep0,))
    got0, got123 = swap(send0, 1), swap(send123, 1)
    parts = combine(levels, others, keep0, keep123, got0, got123, next_own, next_got)
    for_y2 = lax.optimization_barrier(parts[3]) + between(parts[0], 1, (1,))
    arrived = between(parts[1], 2, (0, 1))
    arrived = arrived + between(parts[2], 6, (0, 1))
    own_z = across(parts[0], 0)
    share = between(for_y2, 4, (1,))
    share = share + between(own_z + arrived, 1, (1,))
    share = share + across(parts[3] + arrived, 0)
    north, south = {0: share}, {}
    north[1] = between(share, 1, (1,))
    south[0] = across(share, 1)
    north[4] = between(share, 4, (1,))
    south[2] = between(south[0], 2, (0,))
    south[6] = between(south[0], 6, (0,))
    north[3] = between(north[1], 2, (1,))
    north[7] = between(north[1], 6, (1,))
    north[5] = between(north[4], 1, (1,))
    for slot in (1, 4, 3, 7, 5):
        south[slot] = across(north[slot], 1)
    for slot in (2, 6):
        north[slot] = across(south[slot], 0)
    return restrict(levels, [north[slot] for slot in range(8)] + [south[slot] for slot in range(8)])


def solution(mesh):
    in_specs = (P("grid", "dom", None, None, None, None, None), P("grid", None), P("grid"))
    out_specs = P("grid", "dom", None, None, None, None, None)
    return jax.shard_map(whole, mesh=mesh, in_specs=in_specs, out_specs=out_specs, check_vma=False)
```

```python
import jax
import jax.numpy as jnp
import numpy as np
from jax import lax
from jax.experimental import pallas as pl
from jax.experimental.pallas import tpu as pltpu
from jax.sharding import PartitionSpec as P


TOPS = (5, 2, 2, 3, 3, 7)
FIRST = (5, 3, 7, 4)
SECOND = (1, 2, 6, 0)


def coarse_position(numerator, level_now):
    while numerator > 0 and numerator % 2 == 0:
        numerator = numerator // 2
        level_now = level_now - 1
    if numerator == 0:
        return 0
    return (1 << (level_now - 1)) + (numerator - 1) // 2


def parent_positions(position):
    level_now = position.bit_length()
    span_size = 1 << (level_now - 1)
    offset = position - span_size
    return [
        coarse_position(offset % span_size, level_now - 1),
        coarse_position((offset + 1) % span_size, level_now - 1),
    ]


def interp_tables(top):
    points = 1 << top
    result = []
    for short in range(3):
        matrix = np.eye(points)
        for position in range(points >> short, points):
            first, second = parent_positions(position)
            matrix[position] = 0.5 * (matrix[first] + matrix[second])
        result.append(matrix)
    return np.stack(result)


def two_sources(tables):
    sources = np.zeros((2, *tables.shape[:2]), dtype=np.int32)
    weights = np.zeros((2, *tables.shape[:2]), dtype=np.float32)
    for short in range(tables.shape[0]):
        for row in range(tables.shape[1]):
            found = np.nonzero(tables[short, row])[0]
            for i in range(2):
                at = found[min(i, len(found) - 1)]
                sources[i, short, row] = at
                weights[i, short, row] = tables[short, row, at] if i < len(found) else 0.0
    return sources, weights


def by_shortfall(table, short):
    sublane = lax.broadcasted_iota(jnp.int32, (8, 128), 0)
    kind = np.asarray(table).dtype.type
    result = jnp.full((8, 128), kind(0))
    for row in range(8):
        per = [kind(table[i, row]) for i in range(3)]
        here = jnp.where(short == 0, per[0], jnp.where(short == 1, per[1], per[2]))
        result = jnp.where(sublane == row, here, result)
    return result


def lead_interp(values, top, short):
    result = list(values)
    points = 1 << top
    for missing in (2, 1):
        for position in range(points >> missing, points >> (missing - 1)):
            first, second = parent_positions(position)
            if first == second:
                mean = result[first]
            else:
                mean = 0.5 * (result[first] + result[second])
            result[position] = jnp.where(short >= missing, mean, result[position])
    return result


def interp_kernel(levels, coefs, x, pf, *rest):
    keep, send, done = rest[-3:]
    index = lax.axis_index("grid")
    here, core = jnp.right_shift(index, 1), index & 1
    weight = coefs[0].astype(jnp.float32)
    short = [TOPS[k] - levels[0, k] for k in range(6)]
    matrix = pf[short[5]]
    rows = x[0, 0].reshape(1024, 128)
    high = rows.astype(jnp.bfloat16)
    low = (rows - high.astype(jnp.float32)).astype(jnp.bfloat16)
    along_f = jnp.dot(high, matrix, preferred_element_type=jnp.float32) + jnp.dot(
        low, matrix, preferred_element_type=jnp.float32
    )
    tiles = along_f.reshape(16, 8, 8, 128)
    sources, weights = two_sources(interp_tables(3))
    src1, src2 = (by_shortfall(sources[i], short[4]) for i in range(2))
    wt1, wt2 = (by_shortfall(weights[i], short[4]) * weight for i in range(2))
    by_bc = []
    for bc in range(16):
        along_e = []
        for d in range(8):
            tile = tiles[bc, d]
            along_e.append(
                wt1 * jnp.take_along_axis(tile, src1, axis=0) + wt2 * jnp.take_along_axis(tile, src2, axis=0)
            )
        by_bc.append(lead_interp(along_e, 3, short[3]))
    for d in range(8):
        lines = [lead_interp([by_bc[b * 4 + c][d] for c in range(4)], 2, short[2]) for b in range(4)]
        for c in range(4):
            for b, value in enumerate(lead_interp([lines[b][c] for b in range(4)], 2, short[1])):
                done[b * 4 + c, d] = value
    for i in range(4):
        kept = jnp.where(core == 1, FIRST[i], SECOND[i]) ^ here
        sent = jnp.where(core == 1, SECOND[i], FIRST[i]) ^ here
        for c in range(2):
            for d in range(8):
                keep[i, 0, c, d] = done[kept * 2 + c, d]
                send[i, 0, c, d] = done[sent * 2 + c, d]


def in_vmem(x):
    return pltpu.with_memory_space_constraint(x, pltpu.VMEM)


def in_hbm(x):
    return pltpu.with_memory_space_constraint(x, pltpu.HBM)


def interp_rows(values, levels, coefs, matrices, first, count, after=()):
    smem = pl.BlockSpec(memory_space=pltpu.SMEM)
    half = jax.ShapeDtypeStruct((4, count, 2, 8, 8, 128), jnp.float32)
    out_spec = pl.BlockSpec((4, 1, 2, 8, 8, 128), lambda a: (0, a, 0, 0, 0, 0))
    return pl.pallas_call(
        interp_kernel,
        grid=(count,),
        in_specs=[
            smem,
            smem,
            pl.BlockSpec((1, 1, 4, 4, 8, 8, 128), lambda a: (0, a + first, 0, 0, 0, 0, 0)),
            pl.BlockSpec((3, 128, 128), lambda a: (0, 0, 0)),
            *[pl.BlockSpec(memory_space=pl.ANY) for _ in after],
        ],
        out_specs=[out_spec, out_spec],
        out_shape=[half, half],
        scratch_shapes=[pltpu.VMEM((16, 8, 8, 128), jnp.float32)],
        compiler_params=pltpu.CompilerParams(vmem_limit_bytes=16 << 20),
        cost_estimate=pl.CostEstimate(flops=count * 10**8, bytes_accessed=count << 20, transcendentals=0),
    )(in_hbm(levels), coefs, in_hbm(values), in_hbm(matrices), *after)


def combine_kernel(levels, others, own0, own123, got0, got123, next_own, next_got, *outs):
    short = TOPS[0] - levels[0, 0]
    other_short = TOPS[0] - others[0, 0]
    for at, out in enumerate(outs):
        for c in range(2):
            for d in range(8):
                total = None
                for zero, rest, after, miss in (
                    (own0, own123, next_own, short),
                    (got0, got123, next_got, other_short),
                ):
                    start, end = zero[at, 0, c, d], after[at, 0, c, d]
                    one, two, three = (rest[at, i, c, d] for i in range(3))
                    two = jnp.where(miss >= 2, 0.5 * (start + end), two)
                    one = jnp.where(miss >= 1, 0.5 * (start + two), one)
                    three = jnp.where(miss >= 1, 0.5 * (two + end), three)
                    part = (start, one, two, three)
                    total = part if total is None else tuple(s + t for s, t in zip(total, part))
                for i in range(4):
                    out[i, c, d] = total[i]


def combine(levels, others, *pieces):
    smem = pl.BlockSpec(memory_space=pltpu.SMEM)
    vmem = pl.BlockSpec(memory_space=pltpu.VMEM)
    return pl.pallas_call(
        combine_kernel,
        in_specs=[smem, smem, *[vmem] * len(pieces)],
        out_specs=[vmem] * 4,
        out_shape=[pltpu.VMEM((4, 2, 8, 8, 128), jnp.float32)] * 4,
        compiler_params=pltpu.CompilerParams(vmem_limit_bytes=4 << 20),
        name="combine",
    )(levels, others, *[in_vmem(p) for p in pieces])


def restrict_kernel(levels, *refs):
    north, south, out, scratch, sems = refs[:8], refs[8:16], *refs[16:]
    here = jnp.right_shift(lax.axis_index("grid"), 1)
    short = [TOPS[k] - levels[0, k] for k in range(6)]
    spacing = jnp.left_shift(jnp.int32(1), short[0])
    sublane = lax.broadcasted_iota(jnp.int32, (8, 128), 0)
    lane = lax.broadcasted_iota(jnp.int32, (8, 128), 1)
    inside = (sublane < jnp.right_shift(8, short[4])) & (lane < jnp.right_shift(128, short[5]))
    tile = jnp.where(inside, 1.0, 0.0)
    by_d = [jnp.where(d < jnp.right_shift(8, short[3]), tile, 0.0) for d in range(8)]
    core = lax.axis_index("grid") & 1
    copies = [pltpu.make_async_copy(scratch.at[row], out.at[row], sems.at[row]) for row in range(4)]

    def write(pieces):
        for row in range(4):
            held_a = jnp.where(lax.rem(jnp.int32(row), spacing) == 0, 1.0, 0.0)
            for slot, piece in enumerate(pieces):
                for half in range(2):
                    at = (here ^ slot) * 2 + half
                    b, c = jnp.right_shift(at, 2), at & 3
                    held = jnp.where(
                        (b < jnp.right_shift(4, short[1])) & (c < jnp.right_shift(4, short[2])), held_a, 0.0
                    )
                    for d in range(8):
                        scratch[row, at, d] = piece[row, half, d] * (by_d[d] * held)
            copies[row].start()

    @pl.when(core == 1)
    def _():
        write(north)

    @pl.when(core == 0)
    def _():
        write(south)

    for copy in copies:
        copy.wait()


def restrict(levels, pieces):
    out = pl.pallas_call(
        restrict_kernel,
        in_specs=[pl.BlockSpec(memory_space=pltpu.SMEM)] + [pl.BlockSpec(memory_space=pltpu.VMEM)] * 16,
        out_specs=pl.BlockSpec(memory_space=pl.ANY),
        out_shape=jax.ShapeDtypeStruct((4, 16, 8, 8, 128), jnp.float32),
        scratch_shapes=[pltpu.VMEM((4, 16, 8, 8, 128), jnp.float32), pltpu.SemaphoreType.DMA((4,))],
        compiler_params=pltpu.CompilerParams(vmem_limit_bytes=4 << 20),
        name="restrict",
    )(levels, *[in_vmem(p) for p in pieces])
    return out.reshape(1, 4, 4, 4, 8, 8, 128)


def swap(x, bits):
    return lax.ppermute(x, "grid", [(i, i ^ bits) for i in range(16)])


def between(x, bits, cores):
    pairs = [(h * 2 + core, (h ^ bits if core in cores else h) * 2 + core) for h in range(8) for core in range(2)]
    return lax.ppermute(x, "grid", pairs)


def to_previous(x, bits):
    pairs = [(r * 8 + d, (r ^ bits) * 8 + (d - 1) % 8) for r in range(16) for d in range(8)]
    return lax.ppermute(x, ("grid", "dom"), pairs)


def whole(values, levels, coefficients):
    matrices = jnp.asarray(interp_tables(7).transpose(0, 2, 1), dtype=jnp.bfloat16)
    others = swap(levels, 1)
    keep0, send0 = interp_rows(values, levels, coefficients, matrices, 0, 1)
    next_own = to_previous(keep0, 0)
    next_got = to_previous(send0, 1)
    keep123, send123 = interp_rows(values, levels, coefficients, matrices, 1, 3, (keep0,))
    got0, got123 = swap(send0, 1), swap(send123, 1)
    parts = combine(levels, others, keep0, keep123, got0, got123, next_own, next_got)
    for_y2 = lax.optimization_barrier(parts[3]) + between(parts[0], 1, (1,))
    arrived = between(parts[1], 2, (0, 1))
    arrived = arrived + between(parts[2], 6, (0, 1))
    own_z = swap(parts[0], 1)
    share = between(for_y2, 4, (1,))
    share = share + between(own_z + arrived, 1, (1,))
    share = share + swap(parts[3] + arrived, 1)
    north, south = {0: share}, {}
    north[1] = between(share, 1, (1,))
    south[0] = swap(share, 1)
    north[4] = between(share, 4, (1,))
    south[2] = between(south[0], 2, (0,))
    south[6] = between(south[0], 6, (0,))
    north[3] = between(north[1], 2, (1,))
    north[7] = between(north[1], 6, (1,))
    north[5] = between(north[4], 1, (1,))
    for slot in (1, 4, 3, 7, 5):
        south[slot] = swap(north[slot], 1)
    for slot in (2, 6):
        north[slot] = swap(south[slot], 1)
    return restrict(levels, [north[slot] for slot in range(8)] + [south[slot] for slot in range(8)])


def solution(mesh):
    in_specs = (P("grid", "dom", None, None, None, None, None), P("grid", None), P("grid"))
    out_specs = P("grid", "dom", None, None, None, None, None)
    return jax.shard_map(whole, mesh=mesh, in_specs=in_specs, out_specs=out_specs, check_vma=False)
```
